256 devices in a mesh: param: 64 (over y, z, core), freq: 4 (over x).
Axes of the slice: x: 4, y: 4, z: 8, core: 2. Of those that a mesh axis runs over, the one named last changes fastest.
Arguments:
- kernel_hat: bfloat16 [2, 16, 600, 65536], P(None, 'freq', None, 'param'), may hold values from -0.25 to 0.25
- prior_gain: float32 [16, 65536], P('freq', 'param'), may hold values from 5.722046e-05 to 0.018310547, as said below
- noise_var: float32 [600], replicated, may hold values from 0.5 to 2
- observed: float32 [64, 16, 600], P('param', 'freq'), may hold values from -6 to 6
Outputs:
- solution: float32 [64, 16, 600], P('param', 'freq')
- residual: float32 [64, 16, 600], P('param', 'freq')
The draws below stay inside these ranges and needn't reach their ends.
Inputs may be any that keep to these rules, and one draw needn't show every extreme that they name: `prior_gain`: prior variances are positive.
All inputs are finite; a program needn't handle non-finite values.
Results may differ from the reference program's by a relative error of at most 0.0085.
Values may be sent and summed in bfloat16 or wider, within the bound.
No kernel may reach another device: no remote copies, remote signals or barrier semaphores. Data moves between devices by JAX's collectives and lax.ppermute only.
A program may use at most 64 MiB of HBM per device.

```python
import math
import jax
import jax.numpy as jnp
from jax import lax

NS = 600
NT = 16
P_DEV = 1024
ITERS = 2
NP = 65536
R = 64


def draw_prior_gain(key, part):
    blocks = NP // P_DEV
    first_key, second_key = jax.random.split(jax.random.fold_in(key, 11))
    spread_base = jnp.exp(jax.random.uniform(first_key, (NT, NP), jnp.float32, jnp.log(0.2), jnp.log(2.0)))
    ranking = jax.random.permutation(second_key, blocks)
    weighty = (ranking < 2).astype(jnp.float32)
    factor = 1.0 + weighty * (0.5 * blocks - 1.0)
    overall = 0.5 * NS / (NT * NP)
    return (spread_base * jnp.repeat(factor, P_DEV)[None, :] * overall).astype(jnp.float32)


def shard_levels(rng, dims, shards, smallest, largest):
    factor_of, own = 1.0, jax.random.fold_in(rng, 6)
    for axis_at, shards_of in shards:
        draws = jnp.exp(jax.random.uniform(jax.random.fold_in(own, axis_at), (shards_of,), jnp.float32, smallest / len(shards), largest / len(shards)))
        factor_of = factor_of * jnp.repeat(draws, dims[axis_at] // shards_of).reshape([-1 if axis == axis_at else 1 for axis in range(len(dims))])
    return factor_of


def noise(own_key, shape, deviation, reach, cuts=(), kind=jnp.bfloat16):
    factor_of = shard_levels(own_key, shape, cuts, -0.22, 0.18) if cuts else 1.0
    result = jax.random.normal(own_key, shape, jnp.float32) * deviation * factor_of
    return jnp.minimum(jnp.maximum(result, -reach), reach).astype(kind)


def setup_inputs(seed: int = 0) -> dict:
    streams_of = jax.random.split(jax.random.key(seed), 5)
    return {
        "kernel_hat": noise(streams_of[0], (2, NT, NS, NP), NS ** -0.5, 0.25, ((1, 4), (3, 64))),
        "prior_gain": draw_prior_gain(jax.random.fold_in(streams_of[4], 71), 0),
        "noise_var": jnp.clip(jnp.exp(jax.random.uniform(streams_of[2], (NS,), jnp.float32, math.log(0.5), math.log(2.0))), 0.5, 2.0),
        "observed": noise(streams_of[3], (R, NT, NS), 1.0, 6.0, ((0, 64), (1, 4)), jnp.float32),
    }


HIGHEST = lax.Precision.HIGHEST


def phase_tables(freq_first, freq_count, time_first, time_count, period):
    freq_ids = freq_first + lax.iota(jnp.int32, freq_count)
    time_ids = time_first + lax.iota(jnp.int32, time_count)
    phase_int = (freq_ids[:, None] * time_ids[None, :]) % period
    phase = phase_int.astype(jnp.float32) * (2.0 * math.pi / period)
    return jnp.cos(phase), jnp.sin(phase)


def apply_hessian(fields, kernel_hat, prior_gain, noise_var):
    period = 2 * NT - 1
    cosines, sines = phase_tables(0, NT, 0, NT, period)
    spec_real = jnp.einsum("kt,rts->krs", cosines, fields, precision=HIGHEST).astype(jnp.bfloat16)
    spec_imag = (-jnp.einsum("kt,rts->krs", sines, fields, precision=HIGHEST)).astype(jnp.bfloat16)

    def one_slot(slot_id):
        real_part = kernel_hat[0, slot_id]
        imag_part = kernel_hat[1, slot_id]
        upper = spec_real[slot_id]
        lower = spec_imag[slot_id]
        coef_real = jnp.dot(upper, real_part, preferred_element_type=jnp.float32) + jnp.dot(lower, imag_part, preferred_element_type=jnp.float32)
        coef_imag = jnp.dot(lower, real_part, preferred_element_type=jnp.float32) - jnp.dot(upper, imag_part, preferred_element_type=jnp.float32)
        slot_gain = prior_gain[slot_id]
        coef_real = (coef_real * slot_gain[None, :]).astype(jnp.bfloat16)
        coef_imag = (coef_imag * slot_gain[None, :]).astype(jnp.bfloat16)
        image_real = jnp.dot(coef_real, real_part.T, preferred_element_type=jnp.float32) - jnp.dot(coef_imag, imag_part.T, preferred_element_type=jnp.float32)
        image_imag = jnp.dot(coef_imag, real_part.T, preferred_element_type=jnp.float32) + jnp.dot(coef_real, imag_part.T, preferred_element_type=jnp.float32)
        return image_real, image_imag

    image_real, image_imag = lax.map(one_slot, jnp.arange(NT, dtype=jnp.int32))
    inverse = jnp.einsum("krs,kt->rts", image_real, cosines, precision=HIGHEST) - jnp.einsum("krs,kt->rts", image_imag, sines, precision=HIGHEST)
    return noise_var[None, None, :] * fields + inverse


def reference(kernel_hat, prior_gain, noise_var, observed):
    solution = jnp.zeros_like(observed)
    residual = observed
    direction = observed
    norm_now = jnp.sum(residual * residual, axis=(1, 2))
    for sweep in range(ITERS):
        applied = apply_hessian(direction, kernel_hat, prior_gain, noise_var)
        step_len = norm_now / jnp.sum(direction * applied, axis=(1, 2))
        solution = solution + step_len[:, None, None] * direction
        residual = residual - step_len[:, None, None] * applied
        norm_next = jnp.sum(residual * residual, axis=(1, 2))
        direction = residual + (norm_next / norm_now)[:, None, None] * direction
        norm_now = norm_next
    return solution, residual
```

```python
import math

import jax
import jax.numpy as jnp
from jax import lax
from jax.experimental import pallas as pl
from jax.experimental.pallas import tpu as pltpu
from jax.sharding import PartitionSpec as P

NT = 16
ITERS = 2
PERIOD = 2 * NT - 1

HIGHEST = lax.Precision.HIGHEST
VMEM = pltpu.VMEM
LANES = 128


def one_core_groups(count):
    return [list(range(core, count, 2)) for core in range(2)]


def from_other_core(value):
    count = lax.axis_size("param")
    return lax.ppermute(value, "param", [(i, i ^ 1) for i in range(count)])


def exchange(blocks):
    groups = one_core_groups(lax.axis_size("param"))
    return lax.all_to_all(blocks, "param", 0, 0, axis_index_groups=groups, tiled=True)


def freq_slots(value):
    length = lax.axis_size("freq")
    others = [
        lax.ppermute(value, "freq", [(i, (i + d) % length) for i in range(length)])
        for d in range(1, length)
    ]
    return (value, *others)


def slot_ids(length, each):
    mine = lax.axis_index("freq")
    slots = (mine - lax.iota(jnp.int32, length)) % length
    return (slots[:, None] * each + lax.iota(jnp.int32, each)[None, :]).reshape(-1)


def tables(freq_ids, time_ids):
    phase_int = freq_ids[:, None] * time_ids[None, :] % PERIOD
    phase = phase_int.astype(jnp.float32) * (2.0 * math.pi / PERIOD)
    return jnp.cos(phase), jnp.sin(phase)


def dot_f32(left, right):
    return jnp.dot(left, right, precision=HIGHEST, preferred_element_type=jnp.float32)


def total(value):
    return jnp.sum(jnp.sum(value, axis=0, keepdims=True), axis=1, keepdims=True)


def send_spectra(to_freq_ref, direction, out_ref):
    spectra = dot_f32(to_freq_ref[...], direction).astype(jnp.bfloat16)
    out_ref[...] = jnp.broadcast_to(spectra[None], out_ref.shape)


def first_kernel(to_freq_ref, *refs):
    *slots, out_ref = refs
    observed = jnp.concatenate([slot[...] for slot in slots], axis=0)
    send_spectra(to_freq_ref, observed, out_ref)


def applied_of(to_time_ref, noise_ref, direction, images):
    sensors = direction.shape[1]
    tiles = -(-sensors // LANES)
    each = images[0].shape[0] // tiles
    image = jnp.concatenate(
        [
            jnp.concatenate([slot[i * each : (i + 1) * each] for i in range(tiles)], axis=1)
            for slot in images
        ],
        axis=0,
    )[:, :sensors]
    return noise_ref[...] * direction + dot_f32(to_time_ref[...], image)


def middle_kernel(slots, to_freq_ref, to_time_ref, noise_ref, *refs):
    observed_refs, image_refs = refs[:slots], refs[slots : 2 * slots]
    out_ref, solution_ref, residual_ref, direction_ref, norm_ref = refs[2 * slots :]
    observed = jnp.concatenate([slot[...] for slot in observed_refs], axis=0)
    applied = applied_of(to_time_ref, noise_ref, observed, image_refs)
    norm = total(observed * observed)
    step = norm / total(observed * applied)
    residual = observed - step * applied
    fresh = total(residual * residual)
    direction = residual + (fresh / norm) * observed
    send_spectra(to_freq_ref, direction, out_ref)
    own = solution_ref.shape[0]
    solution_ref[...] = (step * observed)[:own]
    residual_ref[...] = residual[:own]
    direction_ref[...] = direction
    norm_ref[...] = jnp.broadcast_to(fresh, norm_ref.shape)


def last_kernel(to_time_ref, noise_ref, solution_ref, residual_ref, direction_ref, norm_ref, *refs):
    *image_refs, solution_out, residual_out = refs
    direction = direction_ref[...]
    applied = applied_of(to_time_ref, noise_ref, direction, image_refs)
    step = norm_ref[:1, :1] / total(direction * applied)
    own = solution_out.shape[0]
    solution_out[...] = solution_ref[...] + step * direction[:own]
    residual_out[...] = residual_ref[...] - step * applied[:own]


def hessian_kernel(slot_count, kernel_ref, gain_ref, own_ref, other_ref, own_out, other_out):
    slot = pl.program_id(0)
    rows = own_ref.shape[0]
    half = rows // (2 * slot_count)
    row = lax.broadcasted_iota(jnp.int32, (2 * half, rows), 0)
    column = lax.broadcasted_iota(jnp.int32, (2 * half, rows), 1)
    part = (row >= half).astype(jnp.int32)
    wanted = (row - part * half) * (2 * slot_count) + part * slot_count + slot
    pick = (column == wanted).astype(jnp.float32).astype(jnp.bfloat16)
    picked = [
        jnp.dot(pick, ref[...], preferred_element_type=jnp.float32).astype(jnp.bfloat16)
        for ref in (own_ref, other_ref)
    ]
    spectra = jnp.concatenate(picked, axis=0)
    real_part = kernel_ref[0, 0]
    imag_part = kernel_ref[1, 0]
    by_real = jnp.dot(spectra, real_part, preferred_element_type=jnp.float32)
    by_imag = jnp.dot(spectra, imag_part, preferred_element_type=jnp.float32)
    gain = gain_ref[pl.ds(slot, 1), :]
    coeffs = []
    for at in (0, 2 * half):
        upper, lower = slice(at, at + half), slice(at + half, at + 2 * half)
        coeffs.append(((by_real[upper] + by_imag[lower]) * gain).astype(jnp.bfloat16))
        coeffs.append(((by_real[lower] - by_imag[upper]) * gain).astype(jnp.bfloat16))
    coeffs = jnp.concatenate(coeffs, axis=0)
    contract = (((1,), (1,)), ((), ()))
    by_real = lax.dot_general(coeffs, real_part, contract, preferred_element_type=jnp.float32)
    by_imag = lax.dot_general(coeffs, imag_part, contract, preferred_element_type=jnp.float32)
    sensors = by_real.shape[1]
    tiles = -(-sensors // LANES)
    spare = jnp.zeros((half, tiles * LANES - sensors), jnp.float32)
    for at, out in ((0, own_out), (2 * half, other_out)):
        upper, lower = slice(at, at + half), slice(at + half, at + 2 * half)
        images = (by_real[upper] - by_imag[lower], by_real[lower] + by_imag[upper])
        for part, image in enumerate(images):
            image = jnp.concatenate([image, spare], axis=1)
            for tile in range(tiles):
                start = tile * 2 * slot_count + part * slot_count + slot
                out[pl.ds(start, half, stride=2 * slot_count * tiles), :] = image[
                    :, tile * LANES : (tile + 1) * LANES
                ]


def local(kernel_hat, prior_gain, noise_var, observed):
    slot_count, sensors, params = kernel_hat.shape[1:]
    own_times = observed.shape[1]
    freq_size = lax.axis_size("freq")
    half = lax.axis_size("param") // 2
    rows = half * 2 * slot_count
    block = (half, 2 * slot_count, sensors)
    image_rows = -(-sensors // LANES) * 2 * slot_count

    all_ids = slot_ids(freq_size, slot_count)
    time_ids = slot_ids(freq_size, own_times)
    out_cos, out_sin = tables(all_ids[:slot_count], time_ids)
    to_freq = jnp.concatenate([out_cos, -out_sin], axis=0)
    all_cos, all_sin = tables(all_ids, time_ids)
    both = jnp.stack(
        [
            all_cos.reshape(freq_size, slot_count, NT),
            -all_sin.reshape(freq_size, slot_count, NT),
        ],
        axis=1,
    )
    to_time = both.reshape(-1, NT).T
    noise = noise_var[None, :]

    full = pl.BlockSpec(memory_space=VMEM)

    def vmem_call(body, outs, args, name):
        return pl.pallas_call(
            body,
            out_shape=[jax.ShapeDtypeStruct(shape, dtype) for shape, dtype in outs],
            in_specs=[full] * len(args),
            out_specs=[full] * len(outs),
            name=name,
        )(*args)

    def hessian(spectra):
        own = exchange(spectra)
        other = from_other_core(own)
        whole = pl.BlockSpec((rows, sensors), lambda k: (0, 0))
        own_image, other_image = pl.pallas_call(
            lambda *refs: hessian_kernel(slot_count, *refs),
            grid=(slot_count,),
            in_specs=[
                pl.BlockSpec((2, 1, sensors, params), lambda k: (0, k, 0, 0)),
                pl.BlockSpec((slot_count, params), lambda k: (0, 0)),
                whole,
                whole,
            ],
            out_specs=[pl.BlockSpec((half * image_rows, LANES), lambda k: (0, 0))] * 2,
            out_shape=[jax.ShapeDtypeStruct((half * image_rows, LANES), jnp.float32)] * 2,
            name="hessian",
        )(
            kernel_hat,
            prior_gain,
            own.reshape(rows, sensors),
            other.reshape(rows, sensors),
        )
        arrived = from_other_core(other_image)
        partial = (own_image + arrived).reshape(half, image_rows, LANES)
        return freq_slots(exchange(partial).sum(axis=0))

    slots = freq_slots(observed[0])
    spectra = vmem_call(first_kernel, [(block, jnp.bfloat16)], (to_freq, *slots), "first")[0]
    images = hessian(spectra)
    own_shape = ((own_times, sensors), jnp.float32)
    spectra, solution, residual, direction, norm = vmem_call(
        lambda *refs: middle_kernel(freq_size, *refs),
        [
            (block, jnp.bfloat16),
            own_shape,
            own_shape,
            ((NT, sensors), jnp.float32),
            ((8, 128), jnp.float32),
        ],
        (to_freq, to_time, noise, *slots, *images),
        "middle",
    )
    images = hessian(spectra)
    solution, residual = vmem_call(
        last_kernel,
        [own_shape, own_shape],
        (to_time, noise, solution, residual, direction, norm, *images),
        "last",
    )
    return solution[None], residual[None]


def solution(mesh):
    return jax.shard_map(
        local,
        mesh=mesh,
        in_specs=(
            P(None, "freq", None, "param"),
            P("freq", "param"),
            P(),
            P("param", "freq", None),
        ),
        out_specs=(P("param", "freq", None), P("param", "freq", None)),
        check_vma=False,
    )
```

```python
import math

import jax
import jax.numpy as jnp
from jax import lax
from jax.experimental import pallas as pl
from jax.experimental.pallas import tpu as pltpu
from jax.sharding import PartitionSpec as P

NT = 16
ITERS = 2
PERIOD = 2 * NT - 1

HIGHEST = lax.Precision.HIGHEST
VMEM = pltpu.VMEM
LANES = 128
MIB = 1024 * 1024


def one_core_groups(count):
    return [list(range(core, count, 2)) for core in range(2)]


def from_other_core(value):
    count = lax.axis_size("param")
    return lax.ppermute(value, "param", [(i, i ^ 1) for i in range(count)])


def exchange(blocks):
    groups = one_core_groups(lax.axis_size("param"))
    return lax.all_to_all(blocks, "param", 0, 0, axis_index_groups=groups, tiled=True)


def freq_slots(value):
    length = lax.axis_size("freq")
    others = [
        lax.ppermute(value, "freq", [(i, (i + d) % length) for i in range(length)])
        for d in range(1, length)
    ]
    return (value, *others)


def true_id(place, each):
    length = lax.axis_size("freq")
    slot = (lax.axis_index("freq") + length - place // each) % length
    return slot * each + place % each


def phase_table(freq_ids, time_ids, part):
    phase_int = freq_ids * time_ids % PERIOD
    phase = phase_int.astype(jnp.float32) * (2.0 * math.pi / PERIOD)
    return jnp.where(part == 0, jnp.cos(phase), -jnp.sin(phase))


def iota(shape, dim):
    return lax.broadcasted_iota(jnp.int32, shape, dim)


def dot_f32(left, right):
    return jnp.dot(left, right, precision=HIGHEST, preferred_element_type=jnp.float32)


def total(value):
    return jnp.sum(jnp.sum(value, axis=0, keepdims=True), axis=1, keepdims=True)


def send_spectra(to_freq_ref, direction, out_ref):
    spectra = dot_f32(to_freq_ref[...], direction).astype(jnp.bfloat16)
    out_ref[...] = jnp.broadcast_to(spectra[None], out_ref.shape)


def first_kernel(_, to_freq_ref, *refs):
    *slots, out_ref = refs
    observed = jnp.concatenate([slot[...] for slot in slots], axis=0)
    send_spectra(to_freq_ref, observed, out_ref)


def applied_of(to_time_ref, noise_ref, direction, images):
    sensors = direction.shape[1]
    tiles = -(-sensors // LANES)
    each = images[0].shape[0] // tiles
    image = jnp.concatenate(
        [
            jnp.concatenate([slot[i * each : (i + 1) * each] for i in range(tiles)], axis=1)
            for slot in images
        ],
        axis=0,
    )[:, :sensors]
    return noise_ref[...] * direction + dot_f32(to_time_ref[...], image)


def middle_kernel(slots, to_freq_ref, to_time_ref, noise_ref, *refs):
    observed_refs, image_refs = refs[:slots], refs[slots : 2 * slots]
    out_ref, solution_ref, residual_ref, direction_ref, norm_ref = refs[2 * slots :]
    observed = jnp.concatenate([slot[...] for slot in observed_refs], axis=0)
    applied = applied_of(to_time_ref, noise_ref, observed, image_refs)
    norm = total(observed * observed)
    step = norm / total(observed * applied)
    residual = observed - step * applied
    fresh = total(residual * residual)
    direction = residual + (fresh / norm) * observed
    send_spectra(to_freq_ref, direction, out_ref)
    own = solution_ref.shape[0]
    solution_ref[...] = (step * observed)[:own]
    residual_ref[...] = residual[:own]
    direction_ref[...] = direction
    norm_ref[...] = jnp.broadcast_to(fresh, norm_ref.shape)


def last_kernel(to_time_ref, noise_ref, solution_ref, residual_ref, direction_ref, norm_ref, *refs):
    *image_refs, solution_out, residual_out = refs
    direction = direction_ref[...]
    applied = applied_of(to_time_ref, noise_ref, direction, image_refs)
    step = norm_ref[:1, :1] / total(direction * applied)
    own = solution_out.shape[0]
    solution_out[...] = solution_ref[...] + step * direction[:own]
    residual_out[...] = residual_ref[...] - step * applied[:own]


def touch_kernel(*refs):
    out = refs[-1]
    out[...] = jnp.zeros_like(out)


def hessian_kernel(slot_count, kernel_ref, gain_ref, own_ref, other_ref, own_out, other_out):
    rows, sensors = own_ref.shape
    both = rows // slot_count
    half = both // 2
    tiles = -(-sensors // LANES)
    spare = jnp.zeros((half, tiles * LANES - sensors), jnp.float32)
    row = lax.broadcasted_iota(jnp.int32, (rows, rows), 0)
    column = lax.broadcasted_iota(jnp.int32, (rows, rows), 1)
    wanted = row % half * (2 * slot_count) + row // half % 2 * slot_count + row // both
    pick = (column == wanted).astype(jnp.float32).astype(jnp.bfloat16)
    own, other = [
        jnp.dot(pick, ref[...], preferred_element_type=jnp.float32).astype(jnp.bfloat16)
        for ref in (own_ref, other_ref)
    ]
    contract = (((1,), (1,)), ((), ()))

    def forward(slot):
        at = slice(slot * both, (slot + 1) * both)
        spectra = jnp.concatenate([own[at], other[at]], axis=0)
        by_real = jnp.dot(spectra, kernel_ref[0, slot], preferred_element_type=jnp.float32)
        by_imag = jnp.dot(spectra, kernel_ref[1, slot], preferred_element_type=jnp.float32)
        gain = gain_ref[slot : slot + 1, :]
        coeffs = []
        for at in (0, both):
            upper, lower = slice(at, at + half), slice(at + half, at + both)
            coeffs.append(((by_real[upper] + by_imag[lower]) * gain).astype(jnp.bfloat16))
            coeffs.append(((by_real[lower] - by_imag[upper]) * gain).astype(jnp.bfloat16))
        return jnp.concatenate(coeffs, axis=0)

    def backward(slot, coeffs):
        by_real, by_imag = [
            lax.dot_general(
                coeffs, kernel_ref[part, slot], contract, preferred_element_type=jnp.float32
            )
            for part in range(2)
        ]
        for at, out in ((0, own_out), (both, other_out)):
            upper, lower = slice(at, at + half), slice(at + half, at + both)
            images = (by_real[upper] - by_imag[lower], by_real[lower] + by_imag[upper])
            for part, image in enumerate(images):
                image = jnp.concatenate([image, spare], axis=1)
                for tile in range(tiles):
                    start = tile * 2 * slot_count + part * slot_count + slot
                    out[pl.ds(start, half, stride=2 * slot_count * tiles), :] = image[
                        :, tile * LANES : (tile + 1) * LANES
                    ]

    coeffs = forward(0)
    for slot in range(slot_count):
        following = forward(slot + 1) if slot + 1 < slot_count else None
        backward(slot, coeffs)
        coeffs = following


def local(kernel_hat, prior_gain, noise_var, observed):
    slot_count, sensors, params = kernel_hat.shape[1:]
    own_times = observed.shape[1]
    freq_size = lax.axis_size("freq")
    half = lax.axis_size("param") // 2
    rows = half * 2 * slot_count
    block = (half, 2 * slot_count, sensors)
    image_rows = -(-sensors // LANES) * 2 * slot_count

    spectral = 2 * slot_count
    shape = (spectral, NT)
    row = iota(shape, 0)
    to_freq = phase_table(
        true_id(row % slot_count, slot_count),
        true_id(iota(shape, 1), own_times),
        row // slot_count,
    )
    shape = (NT, freq_size * spectral)
    column = iota(shape, 1)
    to_time = phase_table(
        true_id(column // spectral * slot_count + column % slot_count, slot_count),
        true_id(iota(shape, 0), own_times),
        column % spectral // slot_count,
    )
    noise = noise_var[None, :]

    full = pl.BlockSpec(memory_space=VMEM)

    def vmem_call(body, outs, args, name, limit=4, cost=None):
        return pl.pallas_call(
            body,
            out_shape=[jax.ShapeDtypeStruct(shape, dtype) for shape, dtype in outs],
            in_specs=[full] * len(args),
            out_specs=[full] * len(outs),
            compiler_params=pltpu.CompilerParams(vmem_limit_bytes=limit * MIB),
            cost_estimate=cost,
            name=name,
        )(*args)

    def hessian(spectra):
        own = exchange(spectra)
        other = from_other_core(own)
        own_image, other_image = vmem_call(
            lambda *refs: hessian_kernel(slot_count, *refs),
            [((half * image_rows, LANES), jnp.float32)] * 2,
            (
                kernel_hat,
                prior_gain,
                own.reshape(rows, sensors),
                other.reshape(rows, sensors),
            ),
            "hessian",
            16,
        )
        arrived = from_other_core(other_image)
        partial = (own_image + arrived).astype(jnp.bfloat16)
        partials = exchange(partial.reshape(half, image_rows, LANES))
        return freq_slots(partials.astype(jnp.float32).sum(axis=0))

    slots = freq_slots(observed[0])
    touched = vmem_call(
        touch_kernel,
        [((8, 128), jnp.float32)],
        (kernel_hat, to_freq, to_time, noise),
        "touch",
        4,
        pl.CostEstimate(flops=10**10, bytes_accessed=10**7, transcendentals=0),
    )[0]
    spectra = vmem_call(first_kernel, [(block, jnp.bfloat16)], (touched, to_freq, *slots), "first")[0]
    images = hessian(spectra)
    own_shape = ((own_times, sensors), jnp.float32)
    spectra, solution, residual, direction, norm = vmem_call(
        lambda *refs: middle_kernel(freq_size, *refs),
        [
            (block, jnp.bfloat16),
            own_shape,
            own_shape,
            ((NT, sensors), jnp.float32),
            ((8, 128), jnp.float32),
        ],
        (to_freq, to_time, noise, *slots, *images),
        "middle",
    )
    images = hessian(spectra)
    solution, residual = vmem_call(
        last_kernel,
        [own_shape, own_shape],
        (to_time, noise, solution, residual, direction, norm, *images),
        "last",
    )
    return solution[None], residual[None]


def solution(mesh):
    return jax.shard_map(
        local,
        mesh=mesh,
        in_specs=(
            P(None, "freq", None, "param"),
            P("freq", "param"),
            P(),
            P("param", "freq", None),
        ),
        out_specs=(P("param", "freq", None), P("param", "freq", None)),
        check_vma=False,
    )
```

```python
import math

import jax
import jax.numpy as jnp
import numpy as np
from jax import lax
from jax.experimental import pallas as pl
from jax.experimental.pallas import tpu as pltpu
from jax.sharding import PartitionSpec as P

NT = 16
ITERS = 2
PERIOD = 2 * NT - 1

HIGHEST = lax.Precision.HIGHEST
VMEM = pltpu.VMEM
LANES = 128
MIB = 1024 * 1024


def one_core_groups(count):
    size = count // 2
    tall = 8
    order = [(place % (size // tall)) * tall + place // (size // tall) for place in range(size)]
    return [[2 * chip + core for chip in order] for core in range(2)]


def from_other_core(value):
    count = lax.axis_size("param")
    return lax.ppermute(value, "param", [(i, i ^ 1) for i in range(count)])


def exchange(blocks):
    groups = one_core_groups(lax.axis_size("param"))
    return lax.all_to_all(blocks, "param", 0, 0, axis_index_groups=groups, tiled=True)


def freq_slots(value):
    length = lax.axis_size("freq")
    others = [
        lax.ppermute(value, "freq", [(i, (i + d) % length) for i in range(length)])
        for d in range(1, length)
    ]
    return (value, *others)


def transforms(length, each_freq, each_time):
    to_freq, to_time = [], []
    for mine in range(length):
        slots = (mine - np.arange(length)) % length
        freqs = (slots[:, None] * each_freq + np.arange(each_freq)).reshape(-1)
        times = (slots[:, None] * each_time + np.arange(each_time)).reshape(-1)
        phase = (freqs[:, None] * times[None, :] % PERIOD).astype(np.float32)
        phase = (phase * np.float32(2.0 * math.pi / PERIOD)).astype(np.float64)
        both = np.stack([np.cos(phase), -np.sin(phase)]).astype(np.float32)
        to_freq.append(both[:, :each_freq].reshape(2 * each_freq, -1))
        both = both.reshape(2, length, each_freq, -1).transpose(1, 0, 2, 3)
        to_time.append(both.reshape(2 * length * each_freq, -1).T)
    return np.stack(to_freq), np.stack(to_time)


def dot_f32(left, right):
    return jnp.dot(left, right, precision=HIGHEST, preferred_element_type=jnp.float32)


def total(value):
    return jnp.sum(jnp.sum(value, axis=0, keepdims=True), axis=1, keepdims=True)


def send_spectra(mine_ref, to_freq_ref, direction, out_ref):
    spectra = dot_f32(to_freq_ref[mine_ref[0]], direction).astype(jnp.bfloat16)
    out_ref[...] = jnp.broadcast_to(spectra[None], out_ref.shape)


def first_kernel(_, mine_ref, to_freq_ref, *refs):
    *slots, out_ref = refs
    observed = jnp.concatenate([slot[...] for slot in slots], axis=0)
    send_spectra(mine_ref, to_freq_ref, observed, out_ref)


def applied_of(mine_ref, to_time_ref, noise_ref, direction, images):
    sensors = direction.shape[1]
    tiles = -(-sensors // LANES)
    each = images[0].shape[0] // tiles
    image = jnp.concatenate(
        [
            jnp.concatenate([slot[i * each : (i + 1) * each] for i in range(tiles)], axis=1)
            for slot in images
        ],
        axis=0,
    )[:, :sensors]
    return noise_ref[...][None, :] * direction + dot_f32(to_time_ref[mine_ref[0]], image)


def middle_kernel(slots, mine_ref, to_freq_ref, to_time_ref, noise_ref, *refs):
    observed_refs, image_refs = refs[:slots], refs[slots : 2 * slots]
    out_ref, solution_ref, residual_ref, direction_ref, norm_ref = refs[2 * slots :]
    observed = jnp.concatenate([slot[...] for slot in observed_refs], axis=0)
    applied = applied_of(mine_ref, to_time_ref, noise_ref, observed, image_refs)
    norm = total(observed * observed)
    step = norm / total(observed * applied)
    residual = observed - step * applied
    fresh = total(residual * residual)
    direction = residual + (fresh / norm) * observed
    send_spectra(mine_ref, to_freq_ref, direction, out_ref)
    own = solution_ref.shape[0]
    solution_ref[...] = (step * observed)[:own]
    residual_ref[...] = residual[:own]
    direction_ref[...] = direction
    norm_ref[...] = jnp.broadcast_to(fresh, norm_ref.shape)


def last_kernel(mine_ref, to_time_ref, noise_ref, *refs):
    solution_ref, residual_ref, direction_ref, norm_ref, *image_refs, solution_out, residual_out = refs
    direction = direction_ref[...]
    applied = applied_of(mine_ref, to_time_ref, noise_ref, direction, image_refs)
    step = norm_ref[:1, :1] / total(direction * applied)
    own = solution_out.shape[0]
    solution_out[...] = solution_ref[...] + step * direction[:own]
    residual_out[...] = residual_ref[...] - step * applied[:own]


def touch_kernel(_, out_ref):
    out_ref[...] = jnp.zeros_like(out_ref)


def hessian_kernel(slot_count, kernel_ref, gain_ref, own_ref, other_ref, own_out, other_out):
    rows, sensors = own_ref.shape
    both = rows // slot_count
    half = both // 2
    tiles = -(-sensors // LANES)
    spare = jnp.zeros((half, tiles * LANES - sensors), jnp.float32)
    row = lax.broadcasted_iota(jnp.int32, (rows, rows), 0)
    column = lax.broadcasted_iota(jnp.int32, (rows, rows), 1)
    wanted = row % half * (2 * slot_count) + row // half % 2 * slot_count + row // both
    pick = (column == wanted).astype(jnp.float32).astype(jnp.bfloat16)
    own, other = [
        jnp.dot(pick, ref[...], preferred_element_type=jnp.float32).astype(jnp.bfloat16)
        for ref in (own_ref, other_ref)
    ]
    contract = (((1,), (1,)), ((), ()))

    def forward(slot):
        at = slice(slot * both, (slot + 1) * both)
        spectra = jnp.concatenate([own[at], other[at]], axis=0)
        by_real = jnp.dot(spectra, kernel_ref[0, slot], preferred_element_type=jnp.float32)
        by_imag = jnp.dot(spectra, kernel_ref[1, slot], preferred_element_type=jnp.float32)
        gain = gain_ref[slot : slot + 1, :]
        coeffs = []
        for at in (0, both):
            upper, lower = slice(at, at + half), slice(at + half, at + both)
            coeffs.append(((by_real[upper] + by_imag[lower]) * gain).astype(jnp.bfloat16))
            coeffs.append(((by_real[lower] - by_imag[upper]) * gain).astype(jnp.bfloat16))
        return jnp.concatenate(coeffs, axis=0)

    def backward(slot, coeffs):
        by_real, by_imag = [
            lax.dot_general(
                coeffs, kernel_ref[part, slot], contract, preferred_element_type=jnp.float32
            )
            for part in range(2)
        ]
        for at, out in ((0, own_out), (both, other_out)):
            upper, lower = slice(at, at + half), slice(at + half, at + both)
            images = (by_real[upper] - by_imag[lower], by_real[lower] + by_imag[upper])
            for part, image in enumerate(images):
                image = jnp.concatenate([image, spare], axis=1)
                for tile in range(tiles):
                    start = tile * 2 * slot_count + part * slot_count + slot
                    out[pl.ds(start, half, stride=2 * slot_count * tiles), :] = image[
                        :, tile * LANES : (tile + 1) * LANES
                    ]

    coeffs = forward(0)
    for slot in range(slot_count):
        following = forward(slot + 1) if slot + 1 < slot_count else None
        backward(slot, coeffs)
        coeffs = following


def local(kernel_hat, prior_gain, noise_var, observed):
    slot_count, sensors, params = kernel_hat.shape[1:]
    own_times = observed.shape[1]
    freq_size = lax.axis_size("freq")
    half = lax.axis_size("param") // 2
    rows = half * 2 * slot_count
    block = (half, 2 * slot_count, sensors)
    image_rows = -(-sensors // LANES) * 2 * slot_count

    to_freq, to_time = transforms(freq_size, slot_count, own_times)
    mine = lax.axis_index("freq").reshape(1)

    full = pl.BlockSpec(memory_space=VMEM)
    scalar = pl.BlockSpec(memory_space=pltpu.SMEM)

    def vmem_call(body, outs, args, name, limit=4, cost=None):
        return pl.pallas_call(
            body,
            out_shape=[jax.ShapeDtypeStruct(shape, dtype) for shape, dtype in outs],
            in_specs=[scalar if arg is mine else full for arg in args],
            out_specs=[full] * len(outs),
            compiler_params=pltpu.CompilerParams(vmem_limit_bytes=limit * MIB),
            cost_estimate=cost,
            name=name,
        )(*args)

    def hessian(spectra):
        own = exchange(spectra)
        other = from_other_core(own)
        own_image, other_image = vmem_call(
            lambda *refs: hessian_kernel(slot_count, *refs),
            [((half * image_rows, LANES), jnp.float32)] * 2,
            (
                kernel_hat,
                prior_gain,
                own.reshape(rows, sensors),
                other.reshape(rows, sensors),
            ),
            "hessian",
            16,
        )
        arrived = from_other_core(other_image)
        partial = (own_image + arrived).astype(jnp.bfloat16)
        partials = exchange(partial.reshape(half, image_rows, LANES))
        return freq_slots(partials.astype(jnp.float32).sum(axis=0))

    slots = freq_slots(observed[0])
    touched = vmem_call(
        touch_kernel,
        [((8, 128), jnp.float32)],
        (mine,),
        "touch",
        1,
        pl.CostEstimate(flops=10**10, bytes_accessed=10**7, transcendentals=0),
    )[0]
    spectra = vmem_call(first_kernel, [(block, jnp.bfloat16)], (touched, mine, to_freq, *slots), "first")[0]
    images = hessian(spectra)
    own_shape = ((own_times, sensors), jnp.float32)
    spectra, solution, residual, direction, norm = vmem_call(
        lambda *refs: middle_kernel(freq_size, *refs),
        [
            (block, jnp.bfloat16),
            own_shape,
            own_shape,
            ((NT, sensors), jnp.float32),
            ((8, 128), jnp.float32),
        ],
        (mine, to_freq, to_time, noise_var, *slots, *images),
        "middle",
    )
    images = hessian(spectra)
    solution, residual = vmem_call(
        last_kernel,
        [own_shape, own_shape],
        (mine, to_time, noise_var, solution, residual, direction, norm, *images),
        "last",
    )
    return solution[None], residual[None]


def solution(mesh):
    return jax.shard_map(
        local,
        mesh=mesh,
        in_specs=(
            P(None, "freq", None, "param"),
            P("freq", "param"),
            P(),
            P("param", "freq", None),
        ),
        out_specs=(P("param", "freq", None), P("param", "freq", None)),
        check_vma=False,
    )
```

```python
import math

import jax
import jax.numpy as jnp
import numpy as np
from jax import lax
from jax.experimental import pallas as pl
from jax.experimental.pallas import tpu as pltpu
from jax.sharding import PartitionSpec as P

NT = 16
ITERS = 2
PERIOD = 2 * NT - 1

HIGHEST = lax.Precision.HIGHEST
VMEM = pltpu.VMEM
LANES = 128
MIB = 1024 * 1024


def one_core_groups(count):
    size = count // 2
    tall = 8
    order = [(place % (size // tall)) * tall + place // (size // tall) for place in range(size)]
    return [[2 * chip + core for chip in order] for core in range(2)]


def from_other_core(value):
    count = lax.axis_size("param")
    return lax.ppermute(value, "param", [(i, i ^ 1) for i in range(count)])


def exchange(blocks):
    groups = one_core_groups(lax.axis_size("param"))
    return lax.all_to_all(blocks, "param", 0, 0, axis_index_groups=groups, tiled=True)


def freq_slots(value):
    length = lax.axis_size("freq")
    others = [
        lax.ppermute(value, "freq", [(i, (i + d) % length) for i in range(length)])
        for d in range(1, length)
    ]
    return (value, *others)


def transforms(length, slot_count, own_times):
    each = slot_count // 2
    sides = np.arange(2)

    def table(freqs, times):
        phase = (freqs * times % PERIOD).astype(np.float32)
        phase = (phase * np.float32(2.0 * math.pi / PERIOD)).astype(np.float64)
        return np.stack([np.cos(phase), -np.sin(phase)]).astype(np.float32)

    to_freq = np.zeros((length, 2, 2, 2, each, length, 2, own_times), np.float32)
    to_time = np.zeros((length, 2, length, 2, own_times, length, 2, 2, 2, each), np.float32)
    for mine in range(length):
        slots = (mine - np.arange(length)) % length
        times = slots[:, None] * own_times + np.arange(own_times)
        for core in range(2):
            freqs = mine * slot_count + core * each + np.arange(each)
            values = table(freqs[:, None, None], times)
            for side in sides:
                to_freq[mine, core, side, :, :, :, side] = values
            for source in sides:
                first = slots * slot_count + (core + source) % 2 * each
                freqs = first[:, None] + np.arange(each)
                values = table(freqs, times[:, :, None, None]).transpose(1, 2, 3, 0, 4)
                for side in sides:
                    to_time[mine, core, :, side, :, :, source, (side + source) % 2] = values
    rows = 4 * each
    times = 2 * length * own_times
    return (
        to_freq.reshape(length, 2, rows, times),
        to_time.reshape(length, 2, times, 2 * length * rows),
    )


def dot_f32(left, right):
    return jnp.dot(left, right, precision=HIGHEST, preferred_element_type=jnp.float32)


def side_sums(value, own_times):
    rows = jnp.sum(value, axis=1, keepdims=True)
    own = lax.broadcasted_iota(jnp.int32, rows.shape, 0) // own_times % 2 == 0
    sums = [
        jnp.sum(jnp.where(keep, rows, 0.0), axis=0, keepdims=True)
        for keep in (own, jnp.logical_not(own))
    ]
    return jnp.where(own, *sums)


def send_spectra(mine_ref, core_ref, to_freq_ref, direction, out_ref):
    spectra = dot_f32(to_freq_ref[mine_ref[0], core_ref[0]], direction).astype(jnp.bfloat16)
    out_ref[...] = jnp.broadcast_to(spectra[None], out_ref.shape)


def first_kernel(_, mine_ref, core_ref, to_freq_ref, *refs):
    *slots, out_ref = refs
    observed = jnp.concatenate([slot[...] for slot in slots], axis=0)
    send_spectra(mine_ref, core_ref, to_freq_ref, observed, out_ref)


def applied_of(mine_ref, core_ref, to_time_ref, noise_ref, direction, images):
    sensors = direction.shape[1]
    tiles = -(-sensors // LANES)
    rows = to_time_ref.shape[-1] // (2 * len(images))
    image = jnp.concatenate(
        [
            jnp.concatenate(
                [slot[start + i * rows : start + (i + 1) * rows] for i in range(tiles)], axis=1
            )
            for slot in images
            for start in (0, tiles * rows)
        ],
        axis=0,
    )[:, :sensors]
    inverse = dot_f32(to_time_ref[mine_ref[0], core_ref[0]], image)
    return noise_ref[...][None, :] * direction + inverse


def middle_kernel(slots, mine_ref, core_ref, to_freq_ref, to_time_ref, noise_ref, *refs):
    observed_refs, image_refs = refs[:slots], refs[slots : 2 * slots]
    out_ref, solution_ref, residual_ref, direction_ref, norm_ref = refs[2 * slots :]
    own = solution_ref.shape[0]
    observed = jnp.concatenate([slot[...] for slot in observed_refs], axis=0)
    applied = applied_of(mine_ref, core_ref, to_time_ref, noise_ref, observed, image_refs)
    norm = side_sums(observed * observed, own)
    step = norm / side_sums(observed * applied, own)
    residual = observed - step * applied
    fresh = side_sums(residual * residual, own)
    direction = residual + (fresh / norm) * observed
    send_spectra(mine_ref, core_ref, to_freq_ref, direction, out_ref)
    solution_ref[...] = (step * observed)[:own]
    residual_ref[...] = residual[:own]
    direction_ref[...] = direction
    norm_ref[...] = jnp.broadcast_to(fresh[:8], norm_ref.shape)


def last_kernel(mine_ref, core_ref, to_time_ref, noise_ref, *refs):
    solution_ref, residual_ref, direction_ref, norm_ref, *image_refs = refs[:-2]
    solution_out, residual_out = refs[-2:]
    own = solution_out.shape[0]
    direction = direction_ref[...]
    applied = applied_of(mine_ref, core_ref, to_time_ref, noise_ref, direction, image_refs)
    step = norm_ref[:1, :1] / side_sums(direction * applied, own)[:1]
    solution_out[...] = solution_ref[...] + step * direction[:own]
    residual_out[...] = residual_ref[...] - step * applied[:own]


def touch_kernel(*refs):
    out_ref = refs[-1]
    out_ref[...] = jnp.zeros_like(out_ref)


def hessian_kernel(core_ref, *refs):
    own_kernel, other_kernel, own_gain, other_gain, spectra_ref, out_ref = refs
    rows, sensors = spectra_ref.shape
    each = own_kernel.shape[1] // 2
    block = 4 * each
    half = rows // block
    tiles = -(-sensors // LANES)
    spare = jnp.zeros((half, tiles * LANES - sensors), jnp.float32)
    row = lax.broadcasted_iota(jnp.int32, (rows, rows), 0)
    column = lax.broadcasted_iota(jnp.int32, (rows, rows), 1)
    wanted = row % half * block + row // half % 4 * each + row // (4 * half)
    pick = (column == wanted).astype(jnp.float32).astype(jnp.bfloat16)
    picked = jnp.dot(pick, spectra_ref[...], preferred_element_type=jnp.float32)
    picked = picked.astype(jnp.bfloat16)
    contract = (((1,), (1,)), ((), ()))
    base = core_ref[0] * each

    def both_cores(part, slot):
        at = base + slot
        return jnp.concatenate([own_kernel[part, at], other_kernel[part, at]], axis=1)

    def forward(slot):
        spectra = picked[slot * 4 * half : (slot + 1) * 4 * half]
        by_real, by_imag = [
            jnp.dot(spectra, both_cores(part, slot), preferred_element_type=jnp.float32)
            for part in range(2)
        ]
        gain = jnp.concatenate(
            [ref[pl.ds(base + slot, 1), :] for ref in (own_gain, other_gain)], axis=1
        )
        coeffs = []
        for at in (0, 2 * half):
            upper, lower = slice(at, at + half), slice(at + half, at + 2 * half)
            coeffs.append(((by_real[upper] + by_imag[lower]) * gain).astype(jnp.bfloat16))
            coeffs.append(((by_real[lower] - by_imag[upper]) * gain).astype(jnp.bfloat16))
        return jnp.concatenate(coeffs, axis=0)

    def backward(slot, coeffs):
        by_real, by_imag = [
            lax.dot_general(
                coeffs, both_cores(part, slot), contract, preferred_element_type=jnp.float32
            )
            for part in range(2)
        ]
        for side in range(2):
            upper = slice(2 * side * half, (2 * side + 1) * half)
            lower = slice((2 * side + 1) * half, (2 * side + 2) * half)
            images = (by_real[upper] - by_imag[lower], by_real[lower] + by_imag[upper])
            for part, image in enumerate(images):
                image = jnp.concatenate([image, spare], axis=1)
                for tile in range(tiles):
                    start = tile * block + (2 * side + part) * each + slot
                    out_ref[pl.ds(start, half, stride=block * tiles), :] = image[
                        :, tile * LANES : (tile + 1) * LANES
                    ]

    coeffs = forward(0)
    for slot in range(each):
        following = forward(slot + 1) if slot + 1 < each else None
        backward(slot, coeffs)
        coeffs = following


def local(kernel_hat, prior_gain, noise_var, observed):
    slot_count, sensors, params = kernel_hat.shape[1:]
    own_times = observed.shape[1]
    freq_size = lax.axis_size("freq")
    half = lax.axis_size("param") // 2
    block = 2 * slot_count
    rows = half * block
    times = 2 * freq_size * own_times
    image_rows = -(-sensors // LANES) * block
    to_freq, to_time = transforms(freq_size, slot_count, own_times)
    mine = lax.axis_index("freq").reshape(1)
    core = (lax.axis_index("param") & 1).reshape(1)

    full = pl.BlockSpec(memory_space=VMEM)
    scalar = pl.BlockSpec(memory_space=pltpu.SMEM)

    def vmem_call(body, outs, args, name, limit=4, cost=None):
        return pl.pallas_call(
            body,
            out_shape=[jax.ShapeDtypeStruct(shape, dtype) for shape, dtype in outs],
            in_specs=[scalar if arg is mine or arg is core else full for arg in args],
            out_specs=[full] * len(outs),
            compiler_params=pltpu.CompilerParams(vmem_limit_bytes=limit * MIB),
            cost_estimate=cost,
            name=name,
        )(*args)

    def with_other_core(value):
        return jnp.concatenate([value, from_other_core(value)], axis=0)

    other_gain = from_other_core(prior_gain)
    slots = freq_slots(with_other_core(observed[0]))
    touched = vmem_call(
        touch_kernel,
        [((8, 128), jnp.float32)],
        (mine, core),
        "touch",
        1,
        pl.CostEstimate(flops=10**10, bytes_accessed=10**7, transcendentals=0),
    )[0]
    ahead = (kernel_hat, slots[0], other_gain, mine, core)
    other_kernel = from_other_core(lax.optimization_barrier(ahead)[0])

    def hessian(spectra):
        image = vmem_call(
            hessian_kernel,
            [((half * image_rows, LANES), jnp.float32)],
            (
                core,
                kernel_hat,
                other_kernel,
                prior_gain,
                other_gain,
                exchange(spectra).reshape(rows, sensors),
            ),
            "hessian",
            16,
        )[0]
        sent = image.astype(jnp.bfloat16).reshape(half, image_rows, LANES)
        return freq_slots(with_other_core(exchange(sent).astype(jnp.float32).sum(axis=0)))

    ahead = (half, block, sensors)
    spectra = vmem_call(
        first_kernel,
        [(ahead, jnp.bfloat16)],
        (touched, mine, core, to_freq, *slots),
        "first",
    )[0]
    images = hessian(spectra)
    own_shape = ((own_times, sensors), jnp.float32)
    spectra, solution, residual, direction, norm = vmem_call(
        lambda *refs: middle_kernel(freq_size, *refs),
        [
            (ahead, jnp.bfloat16),
            own_shape,
            own_shape,
            ((times, sensors), jnp.float32),
            ((8, 128), jnp.float32),
        ],
        (mine, core, to_freq, to_time, noise_var, *slots, *images),
        "middle",
    )
    images = hessian(spectra)
    solution, residual = vmem_call(
        last_kernel,
        [own_shape, own_shape],
        (mine, core, to_time, noise_var, solution, residual, direction, norm, *images),
        "last",
    )
    return solution[None], residual[None]


def solution(mesh):
    return jax.shard_map(
        local,
        mesh=mesh,
        in_specs=(
            P(None, "freq", None, "param"),
            P("freq", "param"),
            P(),
            P("param", "freq", None),
        ),
        out_specs=(P("param", "freq", None), P("param", "freq", None)),
        check_vma=False,
    )
```

```python
import math

import jax
import jax.numpy as jnp
import numpy as np
from jax import lax
from jax.experimental import pallas as pl
from jax.experimental.pallas import tpu as pltpu
from jax.sharding import PartitionSpec as P

NT = 16
ITERS = 2
PERIOD = 2 * NT - 1

HIGHEST = lax.Precision.HIGHEST
VMEM = pltpu.VMEM
LANES = 128
MIB = 1024 * 1024
CHIP_ORDER = [
    4, 22, 12, 28, 23, 17, 3, 25, 30, 9, 19, 26, 27, 21, 11, 7,
    31, 10, 24, 16, 1, 5, 20, 8, 29, 14, 6, 0, 18, 15, 13, 2,
]


def one_core_groups(count):
    assert sorted(CHIP_ORDER) == list(range(count // 2))
    return [[2 * chip + core for chip in CHIP_ORDER] for core in range(2)]


def from_other_core(value):
    count = lax.axis_size("param")
    return lax.ppermute(value, "param", [(i, i ^ 1) for i in range(count)])


def exchange(blocks):
    groups = one_core_groups(lax.axis_size("param"))
    return lax.all_to_all(blocks, "param", 0, 0, axis_index_groups=groups, tiled=True)


def freq_slots(value):
    length = lax.axis_size("freq")
    others = [
        lax.ppermute(value, "freq", [(i, (i + d) % length) for i in range(length)])
        for d in range(1, length)
    ]
    return (value, *others)


def transforms(length, slot_count, own_times):
    each = slot_count // 2
    sides = np.arange(2)

    def table(freqs, times):
        phase = (freqs * times % PERIOD).astype(np.float32)
        phase = (phase * np.float32(2.0 * math.pi / PERIOD)).astype(np.float64)
        return np.stack([np.cos(phase), -np.sin(phase)]).astype(np.float32)

    to_freq = np.zeros((length, 2, 2, 2, each, length, 2, own_times), np.float32)
    to_time = np.zeros((length, 2, length, 2, own_times, length, 2, 2, 2, each), np.float32)
    for mine in range(length):
        slots = (mine - np.arange(length)) % length
        times = slots[:, None] * own_times + np.arange(own_times)
        for core in range(2):
            freqs = mine * slot_count + core * each + np.arange(each)
            values = table(freqs[:, None, None], times)
            for side in sides:
                to_freq[mine, core, side, :, :, :, side] = values
            for source in sides:
                first = slots * slot_count + (core + source) % 2 * each
                freqs = first[:, None] + np.arange(each)
                values = table(freqs, times[:, :, None, None]).transpose(1, 2, 3, 0, 4)
                for side in sides:
                    to_time[mine, core, :, side, :, :, source, (side + source) % 2] = values
    rows = 4 * each
    times = 2 * length * own_times
    return (
        to_freq.reshape(length, 2, rows, times),
        to_time.reshape(length, 2, times, 2 * length * rows),
    )


def dot_f32(left, right):
    return jnp.dot(left, right, precision=HIGHEST, preferred_element_type=jnp.float32)


def side_sums(value, own_times):
    rows = jnp.sum(value, axis=1, keepdims=True)
    own = lax.broadcasted_iota(jnp.int32, rows.shape, 0) // own_times % 2 == 0
    sums = [
        jnp.sum(jnp.where(keep, rows, 0.0), axis=0, keepdims=True)
        for keep in (own, jnp.logical_not(own))
    ]
    return jnp.where(own, *sums)


def send_spectra(mine_ref, core_ref, to_freq_ref, direction, out_ref):
    spectra = dot_f32(to_freq_ref[mine_ref[0], core_ref[0]], direction).astype(jnp.bfloat16)
    out_ref[...] = jnp.broadcast_to(spectra[None], out_ref.shape)


def first_kernel(_, mine_ref, core_ref, to_freq_ref, *refs):
    *slots, out_ref = refs
    observed = jnp.concatenate([slot[...] for slot in slots], axis=0)
    send_spectra(mine_ref, core_ref, to_freq_ref, observed, out_ref)


def applied_of(mine_ref, core_ref, to_time_ref, noise_ref, direction, images):
    sensors = direction.shape[1]
    tiles = -(-sensors // LANES)
    rows = to_time_ref.shape[-1] // (2 * len(images))
    image = jnp.concatenate(
        [
            jnp.concatenate(
                [slot[start + i * rows : start + (i + 1) * rows] for i in range(tiles)], axis=1
            )
            for slot in images
            for start in (0, tiles * rows)
        ],
        axis=0,
    )[:, :sensors]
    inverse = dot_f32(to_time_ref[mine_ref[0], core_ref[0]], image)
    return noise_ref[...][None, :] * direction + inverse


def middle_kernel(slots, mine_ref, core_ref, to_freq_ref, to_time_ref, noise_ref, *refs):
    observed_refs, image_refs = refs[:slots], refs[slots : 2 * slots]
    out_ref, solution_ref, residual_ref, direction_ref, norm_ref = refs[2 * slots :]
    own = solution_ref.shape[0]
    observed = jnp.concatenate([slot[...] for slot in observed_refs], axis=0)
    applied = applied_of(mine_ref, core_ref, to_time_ref, noise_ref, observed, image_refs)
    norm = side_sums(observed * observed, own)
    step = norm / side_sums(observed * applied, own)
    residual = observed - step * applied
    fresh = side_sums(residual * residual, own)
    direction = residual + (fresh / norm) * observed
    send_spectra(mine_ref, core_ref, to_freq_ref, direction, out_ref)
    solution_ref[...] = (step * observed)[:own]
    residual_ref[...] = residual[:own]
    direction_ref[...] = direction
    norm_ref[...] = jnp.broadcast_to(fresh[:8], norm_ref.shape)


def last_kernel(mine_ref, core_ref, to_time_ref, noise_ref, *refs):
    solution_ref, residual_ref, direction_ref, norm_ref, *image_refs = refs[:-2]
    solution_out, residual_out = refs[-2:]
    own = solution_out.shape[0]
    direction = direction_ref[...]
    applied = applied_of(mine_ref, core_ref, to_time_ref, noise_ref, direction, image_refs)
    step = norm_ref[:1, :1] / side_sums(direction * applied, own)[:1]
    solution_out[...] = solution_ref[...] + step * direction[:own]
    residual_out[...] = residual_ref[...] - step * applied[:own]


def touch_kernel(*refs):
    out_ref = refs[-1]
    out_ref[...] = jnp.zeros_like(out_ref)


def hessian_kernel(core_ref, *refs):
    own_kernel, other_kernel, own_gain, other_gain, spectra_ref, out_ref = refs
    rows, sensors = spectra_ref.shape
    each = own_kernel.shape[1] // 2
    block = 4 * each
    half = rows // block
    tiles = -(-sensors // LANES)
    spare = jnp.zeros((half, tiles * LANES - sensors), jnp.float32)
    row = lax.broadcasted_iota(jnp.int32, (rows, rows), 0)
    column = lax.broadcasted_iota(jnp.int32, (rows, rows), 1)
    wanted = row % half * block + row // half % 4 * each + row // (4 * half)
    pick = (column == wanted).astype(jnp.float32).astype(jnp.bfloat16)
    picked = jnp.dot(pick, spectra_ref[...], preferred_element_type=jnp.float32)
    picked = picked.astype(jnp.bfloat16)
    contract = (((1,), (1,)), ((), ()))
    base = core_ref[0] * each

    def both_cores(part, slot):
        at = base + slot
        return jnp.concatenate([own_kernel[part, at], other_kernel[part, at]], axis=1)

    def forward(slot):
        spectra = picked[slot * 4 * half : (slot + 1) * 4 * half]
        by_real, by_imag = [
            jnp.dot(spectra, both_cores(part, slot), preferred_element_type=jnp.float32)
            for part in range(2)
        ]
        gain = jnp.concatenate(
            [ref[pl.ds(base + slot, 1), :] for ref in (own_gain, other_gain)], axis=1
        )
        coeffs = []
        for at in (0, 2 * half):
            upper, lower = slice(at, at + half), slice(at + half, at + 2 * half)
            coeffs.append(((by_real[upper] + by_imag[lower]) * gain).astype(jnp.bfloat16))
            coeffs.append(((by_real[lower] - by_imag[upper]) * gain).astype(jnp.bfloat16))
        return jnp.concatenate(coeffs, axis=0)

    def backward(slot, coeffs):
        by_real, by_imag = [
            lax.dot_general(
                coeffs, both_cores(part, slot), contract, preferred_element_type=jnp.float32
            )
            for part in range(2)
        ]
        for side in range(2):
            upper = slice(2 * side * half, (2 * side + 1) * half)
            lower = slice((2 * side + 1) * half, (2 * side + 2) * half)
            images = (by_real[upper] - by_imag[lower], by_real[lower] + by_imag[upper])
            for part, image in enumerate(images):
                image = jnp.concatenate([image, spare], axis=1)
                for tile in range(tiles):
                    start = tile * block + (2 * side + part) * each + slot
                    out_ref[pl.ds(start, half, stride=block * tiles), :] = image[
                        :, tile * LANES : (tile + 1) * LANES
                    ]

    coeffs = forward(0)
    for slot in range(each):
        following = forward(slot + 1) if slot + 1 < each else None
        backward(slot, coeffs)
        coeffs = following


def local(kernel_hat, prior_gain, noise_var, observed):
    slot_count, sensors, params = kernel_hat.shape[1:]
    own_times = observed.shape[1]
    freq_size = lax.axis_size("freq")
    half = lax.axis_size("param") // 2
    block = 2 * slot_count
    rows = half * block
    times = 2 * freq_size * own_times
    image_rows = -(-sensors // LANES) * block
    to_freq, to_time = transforms(freq_size, slot_count, own_times)
    mine = lax.axis_index("freq").reshape(1)
    core = (lax.axis_index("param") & 1).reshape(1)

    full = pl.BlockSpec(memory_space=VMEM)
    scalar = pl.BlockSpec(memory_space=pltpu.SMEM)

    def vmem_call(body, outs, args, name, limit=4, cost=None):
        return pl.pallas_call(
            body,
            out_shape=[jax.ShapeDtypeStruct(shape, dtype) for shape, dtype in outs],
            in_specs=[scalar if arg is mine or arg is core else full for arg in args],
            out_specs=[full] * len(outs),
            compiler_params=pltpu.CompilerParams(vmem_limit_bytes=limit * MIB),
            cost_estimate=cost,
            name=name,
        )(*args)

    def with_other_core(value):
        return jnp.concatenate([value, from_other_core(value)], axis=0)

    other_gain = from_other_core(prior_gain)
    slots = freq_slots(with_other_core(observed[0]))
    touched = vmem_call(
        touch_kernel,
        [((8, 128), jnp.float32)],
        (mine, core),
        "touch",
        1,
        pl.CostEstimate(flops=10**10, bytes_accessed=10**7, transcendentals=0),
    )[0]
    ahead = (kernel_hat, slots[0], other_gain, mine, core)
    other_kernel = from_other_core(lax.optimization_barrier(ahead)[0])

    def hessian(spectra):
        image = vmem_call(
            hessian_kernel,
            [((half * image_rows, LANES), jnp.float32)],
            (
                core,
                kernel_hat,
                other_kernel,
                prior_gain,
                other_gain,
                exchange(spectra).reshape(rows, sensors),
            ),
            "hessian",
            16,
        )[0]
        sent = image.astype(jnp.bfloat16).reshape(half, image_rows, LANES)
        return freq_slots(with_other_core(exchange(sent).astype(jnp.float32).sum(axis=0)))

    ahead = (half, block, sensors)
    spectra = vmem_call(
        first_kernel,
        [(ahead, jnp.bfloat16)],
        (touched, mine, core, to_freq, *slots),
        "first",
    )[0]
    images = hessian(spectra)
    own_shape = ((own_times, sensors), jnp.float32)
    spectra, solution, residual, direction, norm = vmem_call(
        lambda *refs: middle_kernel(freq_size, *refs),
        [
            (ahead, jnp.bfloat16),
            own_shape,
            own_shape,
            ((times, sensors), jnp.float32),
            ((8, 128), jnp.float32),
        ],
        (mine, core, to_freq, to_time, noise_var, *slots, *images),
        "middle",
    )
    images = hessian(spectra)
    solution, residual = vmem_call(
        last_kernel,
        [own_shape, own_shape],
        (mine, core, to_time, noise_var, solution, residual, direction, norm, *images),
        "last",
    )
    return solution[None], residual[None]


def solution(mesh):
    return jax.shard_map(
        local,
        mesh=mesh,
        in_specs=(
            P(None, "freq", None, "param"),
            P("freq", "param"),
            P(),
            P("param", "freq", None),
        ),
        out_specs=(P("param", "freq", None), P("param", "freq", None)),
        check_vma=False,
    )
```
